32 devices in a mesh: dp: 8 (over y, x, core), tensor: 4 (over z).
Axes of the slice: x: 2, y: 2, z: 4, core: 2. Of those that a mesh axis runs over, the one named last changes fastest.
Arguments:
- tokens: bfloat16 [2048, 4096], P(('dp', 'tensor')), may hold values from -6 to 6
- gate_weight: bfloat16 [4096, 3584], P('dp', 'tensor'), may hold values from -0.09375 to 0.09375
- up_weight: bfloat16 [4096, 3584], P('dp', 'tensor'), may hold values from -0.09375 to 0.09375
- hidden_cotangent: bfloat16 [2048, 3584], P('dp', 'tensor'), may hold values from -1.5 to 1.5
Outputs:
- hidden: bfloat16 [2048, 3584], P('dp', 'tensor')
- grad_tokens: bfloat16 [2048, 4096], P(('dp', 'tensor'))
- grad_gate: bfloat16 [4096, 3584], P('dp', 'tensor')
- grad_up: bfloat16 [4096, 3584], P('dp', 'tensor')
The draws below stay inside these ranges and needn't reach their ends.
All inputs are finite; a program needn't handle non-finite values.
Results may differ from the reference program's by a relative error of at most 0.023.
Values may be sent and summed in bfloat16 or wider, within the bound.
No kernel may reach another device: no remote copies, remote signals or barrier semaphores. Data moves between devices by JAX's collectives and lax.ppermute only.
A program may use at most 64 MiB of HBM per device.

```python
import jax
import jax.numpy as jnp
from jax import lax

D = 4096
GROUP_TOK = 256
FF = 3584
TOKENS = 2048
N_DP = 8


def with_spikes(result, key, source, target, parts, factor):
    owner, partner = [(jnp.arange(result.shape[dim]) // (result.shape[dim] // parts)).reshape([-1 if axis == dim else 1 for axis in range(result.ndim)]) for dim in (source, target)]
    chosen = jax.random.permutation(key, parts)[partner]
    strong = (owner == chosen) | (owner == (partner + parts // 2) % parts)
    return jnp.where(strong, factor * result, result)


def levels(key, shape, shards, least, largest):
    def one(axis_at, blocks):
        steps = jax.random.uniform(jax.random.fold_in(jax.random.fold_in(key, 6), axis_at), (blocks,), jnp.float32, least / len(shards), largest / len(shards))
        return jnp.repeat(jnp.exp(steps), shape[axis_at] // blocks).reshape((-1,) + (1,) * (len(shape) - axis_at - 1))

    loudness = one(*shards[0])
    for cut in shards[1:]:
        loudness = loudness * one(*cut)
    return loudness


def noise(rng, dims, spread, most, split=(), held_as=jnp.bfloat16):
    values = spread * jax.random.normal(rng, dims, jnp.float32)
    if split:
        values = values * levels(rng, dims, split, -0.22, 0.18)
    return jnp.clip(values, -most, most).astype(held_as)


def bell_draw_with(key, dims, spread, bound, cuts, heavy, kind=jnp.bfloat16):
    result = spread * jax.random.normal(key, dims, jnp.float32)
    if cuts:
        result = result * levels(key, dims, cuts, -0.22, 0.18)
    return jnp.clip(with_spikes(result, jax.random.fold_in(key, 3), *heavy), -bound, bound).astype(kind)


def setup_inputs(seed: int = 0) -> dict:
    key_of = jax.random.split(jax.random.key(seed), 5)
    tokens = bell_draw_with(key_of[0], (TOKENS, D), 1.0, 6.0, ((0, 32),), (0, 1, 32, 2.75))
    gate_weight = noise(key_of[1], (D, FF), D ** -0.5, 0.09375, ((0, 8), (1, 4)))
    up_weight = noise(key_of[2], (D, FF), D ** -0.5, 0.09375, ((0, 8), (1, 4)))
    hidden_cotangent = noise(key_of[3], (TOKENS, FF), 0.25, 1.5, ((0, 8), (1, 4)))
    return {"tokens": tokens, "gate_weight": gate_weight, "up_weight": up_weight, "hidden_cotangent": hidden_cotangent}


def swiglu_parts(gate_pre, up_pre, cotangent):
    sigmoid_val = jax.nn.sigmoid(gate_pre)
    activation = gate_pre * sigmoid_val
    hidden = (activation * up_pre).astype(jnp.bfloat16)
    upstream = cotangent.astype(jnp.float32)
    slope = sigmoid_val * (1.0 + gate_pre * (1.0 - sigmoid_val))
    grad_gate_pre = (upstream * up_pre * slope).astype(jnp.bfloat16)
    grad_up_pre = (upstream * activation).astype(jnp.bfloat16)
    return hidden, grad_gate_pre, grad_up_pre


def reference(tokens, gate_weight, up_weight, hidden_cotangent):
    gate_pre = jnp.dot(tokens, gate_weight, preferred_element_type=jnp.float32)
    up_pre = jnp.dot(tokens, up_weight, preferred_element_type=jnp.float32)
    hidden, grad_gate_pre, grad_up_pre = swiglu_parts(gate_pre, up_pre, hidden_cotangent)
    input_sum = jnp.dot(grad_gate_pre, gate_weight.T, preferred_element_type=jnp.float32)
    input_sum = input_sum + jnp.dot(grad_up_pre, up_weight.T, preferred_element_type=jnp.float32)
    grad_tokens = input_sum.astype(jnp.bfloat16)
    joined = jnp.concatenate([grad_gate_pre, grad_up_pre], axis=1)

    def add_group(carry, group_index):
        first_row = (group_index * GROUP_TOK).astype(jnp.int32)
        rows_part = lax.dynamic_slice_in_dim(tokens, first_row, GROUP_TOK, 0)
        grads_part = lax.dynamic_slice_in_dim(joined, first_row, GROUP_TOK, 0)
        term = jnp.dot(rows_part.T, grads_part, preferred_element_type=jnp.float32)
        term = lax.optimization_barrier(term.astype(jnp.bfloat16)).astype(jnp.float32)
        return carry + term, None

    total, _ = lax.scan(add_group, jnp.zeros((D, 2 * FF), jnp.float32), jnp.arange(N_DP, dtype=jnp.int32))
    grad_gate = total[:, :FF].astype(jnp.bfloat16)
    grad_up = total[:, FF:].astype(jnp.bfloat16)
    return hidden, grad_tokens, grad_gate, grad_up
```

```python
import jax
import jax.numpy as jnp
from jax import lax
from jax.sharding import PartitionSpec as P


def swiglu_parts(gate_pre, up_pre, cotangent):
    sigmoid_val = jax.nn.sigmoid(gate_pre)
    activation = gate_pre * sigmoid_val
    hidden = (activation * up_pre).astype(jnp.bfloat16)
    upstream = cotangent.astype(jnp.float32)
    slope = sigmoid_val * (1.0 + gate_pre * (1.0 - sigmoid_val))
    grad_gate_pre = (upstream * up_pre * slope).astype(jnp.bfloat16)
    grad_up_pre = (upstream * activation).astype(jnp.bfloat16)
    return (hidden, grad_gate_pre, grad_up_pre)


def pick(index, choices):
    result = choices[0]
    for place, choice in enumerate(choices[1:], 1):
        result = jnp.where(index == place, choice, result)
    return result


def swap(value, axis, mask):
    size = lax.axis_size(axis)
    return lax.ppermute(value, axis, [(i, i ^ mask) for i in range(size)])


def bits_of(count):
    return [1 << i for i in range(count.bit_length() - 1)]


def scatter_sum(blocks, bits):
    held = dict(enumerate(blocks))
    for bit in bits:
        sent = [m for m in held if m & bit]
        rows = held[sent[0]].shape[0]
        joined = jnp.concatenate([held[m].astype(jnp.bfloat16) for m in sent], axis=0)
        got = swap(joined, "dp", 2 * bit)
        for place, m in enumerate(sent):
            del held[m]
            term = got[place * rows : (place + 1) * rows].astype(jnp.float32)
            held[m ^ bit] = held[m ^ bit].astype(jnp.float32) + term
    return held[0]


def gather_all(block, bits):
    held = {0: block}
    rows = block.shape[0]
    for bit in bits:
        order = sorted(held)
        got = swap(jnp.concatenate([held[m] for m in order], axis=0), "dp", 2 * bit)
        for place, m in enumerate(order):
            held[m | bit] = got[place * rows : (place + 1) * rows]
    return [held[m] for m in sorted(held)]


def body(tokens, gate_weight, up_weight, hidden_cotangent):
    chips = lax.axis_size("dp") // 2
    planes = lax.axis_size("tensor")
    chip = lax.axis_index("dp") // 2
    core = lax.axis_index("dp") % 2
    plane = lax.axis_index("tensor")
    rows, width = tokens.shape[0], gate_weight.shape[1]
    depth = 2 * gate_weight.shape[0]
    bits = bits_of(chips)

    slices = [tokens[:, i * depth : (i + 1) * depth] for i in range(chips)]
    near = [pick(chip ^ m, slices) for m in range(chips)]
    near = [near[0]] + [swap(near[m], "dp", 2 * m) for m in range(1, chips)]
    own_rows = jnp.concatenate(near, axis=0)
    features = [own_rows] + [swap(own_rows, "tensor", m) for m in range(1, planes)]

    joined = jnp.concatenate([gate_weight, up_weight], axis=1)
    other = swap(joined, "dp", 1)
    weight = jnp.concatenate(
        [jnp.where(core == 0, joined, other), jnp.where(core == 0, other, joined)], axis=0
    )

    hidden = jnp.zeros((planes * rows, width), jnp.bfloat16)
    grads, terms = [], []
    for m in range(planes):
        order = bits if m % 2 == 0 else bits[::-1]
        partial = jnp.dot(features[m], weight, preferred_element_type=jnp.float32).astype(jnp.bfloat16)
        both = scatter_sum([partial[i * rows : (i + 1) * rows] for i in range(chips)], order)
        first = (plane ^ m) * rows
        part, grad_gate_pre, grad_up_pre = swiglu_parts(
            both[:, :width],
            both[:, width:],
            lax.dynamic_slice_in_dim(hidden_cotangent, first, rows, 0),
        )
        hidden = lax.dynamic_update_slice_in_dim(hidden, part, first, 0)
        every = jnp.concatenate(
            gather_all(jnp.concatenate([grad_gate_pre, grad_up_pre], axis=1), order), axis=0
        )
        grads.append(every)
        term = jnp.einsum("tf,df->td", every, weight, preferred_element_type=jnp.float32)
        terms.append(term if m == 0 else swap(term.astype(jnp.bfloat16), "tensor", m))
    total = terms[0]
    for term in terms[1:]:
        total = total + term.astype(jnp.float32)
    total = total.astype(jnp.bfloat16)
    mine = [total[:rows]] + [
        swap(total[m * rows : (m + 1) * rows], "dp", 2 * m) for m in range(1, chips)
    ]
    input_rows = jnp.concatenate(
        [pick(chip ^ i, mine) for i in range(chips)], axis=1
    )

    weight_terms = jnp.einsum(
        "td,tf->df",
        jnp.concatenate(features, axis=0),
        jnp.concatenate(grads, axis=0),
        preferred_element_type=jnp.float32,
    )
    low, high = weight_terms[: depth // 2], weight_terms[depth // 2 :]
    given = jnp.where(core == 0, high, low).astype(jnp.bfloat16)
    kept = jnp.where(core == 0, low, high)
    weight_total = (kept + swap(given, "dp", 1).astype(jnp.float32)).astype(jnp.bfloat16)
    return (hidden, input_rows, weight_total[:, :width], weight_total[:, width:])


def solution(mesh):
    placed = (P(("dp", "tensor"), None), P("dp", "tensor"), P("dp", "tensor"), P("dp", "tensor"))
    return jax.shard_map(
        body,
        mesh=mesh,
        in_specs=placed,
        out_specs=(
            P("dp", "tensor"),
            P(("dp", "tensor"), None),
            P("dp", "tensor"),
            P("dp", "tensor"),
        ),
        check_vma=False,
    )
```
